16 devices in a mesh: dp: 2 (over y, z), sp: 8 (over x, core).
Axes of the slice: x: 4, y: 2, z: 1, core: 2. Of those that a mesh axis runs over, the one named last changes fastest.
The devices are a block of a 4x4x8 slice.
Arguments:
- x_patch: bfloat16 [64, 4096, 768], P('dp', 'sp'), parts along dimension 0
- w_tok1: bfloat16 [4096, 384], P('sp')
- b_tok1: float32 [384], P('sp')
- w_tok2: bfloat16 [384, 4096], P(None, 'sp')
- b_tok2: float32 [4096], P('sp')
- w_ch1: bfloat16 [768, 3072], replicated
- b_ch1: float32 [3072], replicated
- w_ch2: bfloat16 [3072, 768], replicated
- b_ch2: float32 [768], replicated
- ln1_gain: float32 [768], replicated
- ln1_bias: float32 [768], replicated
- ln2_gain: float32 [768], replicated
- ln2_bias: float32 [768], replicated
Outputs:
- output: bfloat16 [64, 4096, 768], P('dp', 'sp'), parts along dimension 0
There are 2 independent parts. The reference program is written for one: setup_inputs(seed, part) draws one part's arguments, and reference() takes and returns one part's arrays. A program takes and returns all parts, laid end to end along the dimension named above; an argument that names none is the same for every part.
All inputs are finite; a program needn't handle non-finite values.
Results may differ from the reference program's by a relative error of at most 0.00985338.
Values are sent between devices in bfloat16 or wider.
A program may use at most 768 MiB of HBM per device.

```python
import jax
import jax.numpy as jnp
from jax import lax

BATCH = 32
PATCHES = 4096
CHANNELS = 768
TOKEN_HID = 384
CHAN_HID = 3072
LN_EPS = 1e-6


def draw_normal(rng_key, out_shape, spread):
    return jax.random.normal(rng_key, out_shape, jnp.float32) * spread


def setup_inputs(seed: int = 0, part: int = 0) -> dict:
    shared = jax.random.split(jax.random.key(seed), 12)
    x_key = jax.random.fold_in(jax.random.key(seed + 1), part)
    x_patch = jax.random.normal(x_key, (BATCH, PATCHES, CHANNELS), jnp.float32)
    return {
        "x_patch": x_patch.astype(jnp.bfloat16),
        "w_tok1": draw_normal(shared[0], (PATCHES, TOKEN_HID), PATCHES ** -0.5).astype(jnp.bfloat16),
        "b_tok1": draw_normal(shared[1], (TOKEN_HID,), 0.5),
        "w_tok2": draw_normal(shared[2], (TOKEN_HID, PATCHES), TOKEN_HID ** -0.5).astype(jnp.bfloat16),
        "b_tok2": draw_normal(shared[3], (PATCHES,), 0.5),
        "w_ch1": draw_normal(shared[4], (CHANNELS, CHAN_HID), CHANNELS ** -0.5).astype(jnp.bfloat16),
        "b_ch1": draw_normal(shared[5], (CHAN_HID,), 0.5),
        "w_ch2": draw_normal(shared[6], (CHAN_HID, CHANNELS), CHAN_HID ** -0.5).astype(jnp.bfloat16),
        "b_ch2": draw_normal(shared[7], (CHANNELS,), 0.3),
        "ln1_gain": 1.0 + draw_normal(shared[8], (CHANNELS,), 0.2),
        "ln1_bias": draw_normal(shared[9], (CHANNELS,), 0.3),
        "ln2_gain": 1.0 + draw_normal(shared[10], (CHANNELS,), 0.2),
        "ln2_bias": draw_normal(shared[11], (CHANNELS,), 0.3),
    }


def layer_norm(values, ln_gain, ln_bias):
    mean_val = jnp.mean(values, axis=-1, keepdims=True)
    centred = values - mean_val
    var_val = jnp.mean(centred * centred, axis=-1, keepdims=True)
    return centred * lax.rsqrt(var_val + LN_EPS) * ln_gain + ln_bias


def reference(x_patch, w_tok1, b_tok1, w_tok2, b_tok2, w_ch1, b_ch1, w_ch2, b_ch2, ln1_gain, ln1_bias, ln2_gain, ln2_bias):
    def one_image(x_img):
        x_wide = x_img.astype(jnp.float32)
        normed = layer_norm(x_wide, ln1_gain, ln1_bias).astype(jnp.bfloat16)
        tok_pre = jnp.dot(w_tok1.T, normed, preferred_element_type=jnp.float32) + b_tok1[:, None]
        tok_act = jax.nn.gelu(tok_pre).astype(jnp.bfloat16)
        tok_out = jnp.dot(w_tok2.T, tok_act, preferred_element_type=jnp.float32) + b_tok2[:, None]
        x_mid = (x_wide + tok_out).astype(jnp.bfloat16)
        mid_wide = x_mid.astype(jnp.float32)
        normed_two = layer_norm(mid_wide, ln2_gain, ln2_bias).astype(jnp.bfloat16)
        ch_pre = jnp.dot(normed_two, w_ch1, preferred_element_type=jnp.float32) + b_ch1
        ch_act = jax.nn.gelu(ch_pre).astype(jnp.bfloat16)
        ch_out = jnp.dot(ch_act, w_ch2, preferred_element_type=jnp.float32) + b_ch2
        return (mid_wide + ch_out).astype(jnp.bfloat16)

    return lax.map(one_image, x_patch)
```

```python
import functools

import jax
import jax.numpy as jnp
from jax import lax
from jax.experimental import pallas as pl
from jax.experimental.pallas import tpu as pltpu
from jax.sharding import PartitionSpec as P

LN_EPS = 1e-6
GELU_A = 0.7978845608028654
GELU_B = 0.7978845608028654 * 0.044715


def gelu(v):
    inner = v * (GELU_A + GELU_B * (v * v))
    return (0.5 * v) * (1.0 + jnp.tanh(inner))


def layer_norm(values, gain, bias):
    width = values.shape[-1]
    mean = jnp.sum(values, axis=-1, keepdims=True) * (1.0 / width)
    centred = values - mean
    var = jnp.sum(centred * centred, axis=-1, keepdims=True) * (1.0 / width)
    return centred * lax.rsqrt(var + LN_EPS) * gain + bias


def dot(a, b):
    return lax.dot_general(a, b, (((1,), (0,)), ((), ())), preferred_element_type=jnp.float32)


def first_kernel(x_ref, w_ref, gain_ref, bias_ref, o_ref, u_ref):
    rows = x_ref.shape[1]
    for r in range(0, rows, 64):
        xs = x_ref[0, r:r + 64, :].astype(jnp.float32)
        u_ref[r:r + 64, :] = layer_norm(xs, gain_ref[...], bias_ref[...]).astype(jnp.bfloat16)
    o_ref[0] = dot(w_ref[...], u_ref[...])


def first_call(x, w1t, gain, bias):
    n, s, c = x.shape
    d = w1t.shape[0]
    return pl.pallas_call(
        first_kernel,
        grid=(n,),
        out_shape=jax.ShapeDtypeStruct((n, d, c), jnp.float32),
        in_specs=[
            pl.BlockSpec((1, s, c), lambda i: (i, 0, 0)),
            pl.BlockSpec((d, s), lambda i: (0, 0)),
            pl.BlockSpec((1, c), lambda i: (0, 0)),
            pl.BlockSpec((1, c), lambda i: (0, 0)),
        ],
        out_specs=pl.BlockSpec((1, d, c), lambda i: (i, 0, 0)),
        scratch_shapes=[pltpu.VMEM((s, c), jnp.bfloat16)],
    )(x, w1t, gain, bias)


def second_kernel(n_img, x_hbm, g_hbm, w2t_hbm, wc1_hbm, wc2_hbm, b2_ref, bc1_ref, bc2_ref, gain_ref, bias_ref, z_hbm,
                  xb, gb, zb, w2t, wc1, wc2, tbuf, x1, vn, v, a0, a1, a2, acc, sem_x, sem_g, sem_z, sem_w):
    def load_x(i):
        return pltpu.make_async_copy(x_hbm.at[i], xb.at[lax.rem(i, 2)], sem_x.at[lax.rem(i, 2)])

    def load_g(i):
        return pltpu.make_async_copy(g_hbm.at[i], gb.at[lax.rem(i, 2)], sem_g.at[lax.rem(i, 2)])

    def store_z(i):
        return pltpu.make_async_copy(zb.at[lax.rem(i, 2)], z_hbm.at[i], sem_z.at[lax.rem(i, 2)])

    weights = [pltpu.make_async_copy(s, d, sem_w.at[k]) for k, (s, d) in enumerate(
        [(w2t_hbm, w2t), (wc1_hbm, wc1), (wc2_hbm, wc2)])]
    load_x(0).start()
    load_g(0).start()
    for w in weights:
        w.start()
    load_x(1).start()
    load_g(1).start()

    rows = x1.shape[0]
    abufs = (a0, a1, a2)
    wide = a0.shape[1]

    def token_mix(slot):
        gv = gb[slot]
        for c in range(0, 768, 256):
            tbuf[:, c:c + 256] = dot(w2t[...], gv[:, c:c + 256])
        for r in range(0, rows, 64):
            xs = xb[slot, r:r + 64, :].astype(jnp.float32)
            x_mid = (xs + (tbuf[r:r + 64, :] + b2_ref[r:r + 64, :])).astype(jnp.bfloat16)
            x1[r:r + 64, :] = x_mid
            vn[r:r + 64, :] = layer_norm(x_mid.astype(jnp.float32), gain_ref[...], bias_ref[...]).astype(jnp.bfloat16)

    def p1(s, src):
        for c in range(0, wide, 256):
            k = s * wide + c
            pre = dot(src[...], wc1[:, k:k + 256]) + bc1_ref[:, k:k + 256]
            abufs[s][:, c:c + 256] = gelu(pre).astype(jnp.bfloat16)

    def p2(s, slot=None):
        for c in range(0, 768, 256):
            part = dot(abufs[s][...], wc2[s * wide:(s + 1) * wide, c:c + 256])
            if s == 0:
                acc[:, c:c + 256] = part + (x1[:, c:c + 256].astype(jnp.float32) + bc2_ref[:, c:c + 256])
            elif s == 1:
                acc[:, c:c + 256] += part
            else:
                zb[slot, :, c:c + 256] = (acc[:, c:c + 256] + part).astype(jnp.bfloat16)

    load_x(0).wait()
    load_g(0).wait()
    weights[0].wait()
    token_mix(0)
    weights[1].wait()
    weights[2].wait()

    def body(n, _):
        prev = n - 1
        slot = lax.rem(n + 1, 2)

        @pl.when(n >= 3)
        def _():
            store_z(n - 3).wait()

        p1(0, vn)
        v[...] = vn[...]
        p2(2, slot)
        @pl.when(n >= 1)
        def _():
            store_z(prev).start()

        @pl.when(n + 1 < n_img)
        def _():
            load_x(n + 1).wait()
            load_g(n + 1).wait()

        p1(1, v)
        p2(0)
        p1(2, v)
        p2(1)
        token_mix(slot)

        @pl.when(n + 2 < n_img)
        def _():
            load_x(n + 2).start()
            load_g(n + 2).start()

        return 0

    lax.fori_loop(0, n_img, body, 0)
    last = n_img - 1
    store_z(last - 2).wait()
    p2(2, last % 2)
    store_z(last).start()
    store_z(last - 1).wait()
    store_z(last).wait()


def second_call(x, g, w2t, wc1, wc2, b2, bc1, bc2, gain, bias):
    n, s, c = x.shape
    d = g.shape[1]
    f = wc1.shape[1]
    any_spec = pl.BlockSpec(memory_space=pl.ANY)
    vm = pl.BlockSpec(memory_space=pltpu.VMEM)
    bf, f32 = jnp.bfloat16, jnp.float32
    return pl.pallas_call(
        functools.partial(second_kernel, n),
        out_shape=jax.ShapeDtypeStruct((n, s, c), bf),
        in_specs=[any_spec] * 5 + [vm] * 5,
        out_specs=any_spec,
        scratch_shapes=[
            pltpu.VMEM((2, s, c), bf), pltpu.VMEM((2, d, c), bf), pltpu.VMEM((2, s, c), bf),
            pltpu.VMEM((s, d), bf), pltpu.VMEM((c, f), bf), pltpu.VMEM((f, c), bf),
            pltpu.VMEM((s, c), f32), pltpu.VMEM((s, c), bf), pltpu.VMEM((s, c), bf), pltpu.VMEM((s, c), bf),
            pltpu.VMEM((s, f // 3), bf), pltpu.VMEM((s, f // 3), bf), pltpu.VMEM((s, f // 3), bf),
            pltpu.VMEM((s, c), f32),
            pltpu.SemaphoreType.DMA((2,)), pltpu.SemaphoreType.DMA((2,)), pltpu.SemaphoreType.DMA((2,)),
            pltpu.SemaphoreType.DMA((3,)),
        ],
        compiler_params=pltpu.CompilerParams(vmem_limit_bytes=60 * 1024 * 1024),
    )(x, g, w2t, wc1, wc2, b2, bc1, bc2, gain, bias)


def solution(mesh):
    row_spec = P("dp", "sp", None)

    def local_layer(x_blk, w1_rows, b1_part, w2_cols, b2_part, w_ch1, b_ch1, w_ch2, b_ch2, ln1_gain, ln1_bias, ln2_gain, ln2_bias):
        part_pre = first_call(x_blk, w1_rows.T, ln1_gain[None], ln1_bias[None])
        tok_pre = lax.psum_scatter(part_pre, "sp", scatter_dimension=1, tiled=True) + b1_part[None, :, None]
        tok_act = gelu(tok_pre).astype(jnp.bfloat16)
        act_full = lax.all_gather(tok_act, "sp", axis=1, tiled=True)
        return second_call(x_blk, act_full, w2_cols.T, w_ch1, w_ch2, b2_part[:, None], b_ch1[None], b_ch2[None],
                           ln2_gain[None], ln2_bias[None])

    in_specs = (row_spec, P("sp", None), P("sp"), P(None, "sp"), P("sp"), P(None, None), P(None), P(None, None), P(None), P(None), P(None), P(None), P(None))
    return jax.shard_map(local_layer, mesh=mesh, in_specs=in_specs, out_specs=row_spec, check_vma=False)
```

```python
import functools

import jax
import jax.numpy as jnp
from jax import lax
from jax.experimental import pallas as pl
from jax.experimental.pallas import tpu as pltpu
from jax.sharding import PartitionSpec as P

LN_EPS = 1e-6
GELU_A = 0.7978845608028654
GELU_B = 0.7978845608028654 * 0.044715
BF, F32 = jnp.bfloat16, jnp.float32
SLOTS = 8
SEND_PAIR, SUM_PAIR, SEND_FAR, SUM_FAR, SEND_NEAR, SUM_NEAR = 1, 2, 3, 4, 5, 7
SEND_ACT, FORWARD, FORWARD_FAR, TOKEN, MAIN = 8, 10, 11, 12, 13


def gelu(v):
    inner = v * (GELU_A + GELU_B * (v * v))
    return (0.5 * v) * (1.0 + jnp.tanh(inner))


def layer_norm(values, gain, bias):
    width = values.shape[-1]
    mean = jnp.sum(values, axis=-1, keepdims=True) * (1.0 / width)
    centred = values - mean
    var = jnp.sum(centred * centred, axis=-1, keepdims=True) * (1.0 / width)
    return centred * lax.rsqrt(var + LN_EPS) * gain + bias


def dot(a, b):
    return lax.dot_general(a, b, (((1,), (0,)), ((), ())), preferred_element_type=F32)


def kernel(n_img, x_hbm, w1t_hbm, w2t_hbm, wc1_hbm, wc2_hbm, b1_ref, b2_ref, bc1_ref, bc2_ref,
           gain1_ref, bias1_ref, gain2_ref, bias2_ref, z_hbm,
           xa, xt, zb, w1p, w2t, wc1, wc2, u, own, pair_out, pair_in, q0, q1, far_out, far_in, near_out, near_in, act,
           tbuf, x1, vn, v, a0, a1, a2, acc, sem_xa, sem_xt, sem_z, sem_w, send_sems, recv_sems):
    rows, chan = x1.shape
    half = chan // 2
    part = act.shape[2]
    n_dev = act.shape[1]
    me = lax.axis_index("sp")
    core = lax.rem(me, 2)
    sib = me + 1 - 2 * core
    up = lax.rem(me + 2, n_dev)
    down = lax.rem(me + n_dev - 2, n_dev)
    far = lax.rem(me + 4, n_dev)

    def s8(i):
        return lax.rem(i, SLOTS)

    def s4(i):
        return lax.rem(i, 4)

    def remote(kind, i, src, dst, to):
        return pltpu.make_async_remote_copy(
            src_ref=src, dst_ref=dst, send_sem=send_sems.at[kind, s8(i)], recv_sem=recv_sems.at[kind, s8(i)],
            device_id={"sp": to}, device_id_type=pl.DeviceIdType.MESH)

    lo, hi = pl.ds(0, half), pl.ds(half, half)

    def out_pair(i):
        return [remote(0, i, pair_out.at[s4(i)], pair_in.at[s8(i)], sib)]

    def out_far(i):
        return [remote(1, i, far_out.at[s4(i), 0], far_in.at[s8(i), 0], up),
                remote(2, i, far_out.at[s4(i), 1], far_in.at[s8(i), 1], down)]

    def out_near(i):
        return [remote(3, i, near_out.at[s4(i), 0], near_in.at[s8(i), 0], up),
                remote(4, i, near_out.at[s4(i), 1], near_in.at[s8(i), 1], down)]

    def block(i, k):
        return act.at[s8(i), k]

    def out_act(i):
        b = block(i, me)
        return [remote(5, i, b, b, up), remote(6, i, b, b, down), remote(7, i, b, b, sib)]

    def out_forward(i):
        lower, upper = block(i, down), block(i, up)
        lower_half, upper_half = act.at[s8(i), down, :, lo], act.at[s8(i), up, :, hi]
        return [remote(8, i, lower_half, lower_half, up), remote(9, i, upper_half, upper_half, down),
                remote(10, i, lower, lower, sib), remote(11, i, upper, upper, sib)]

    def out_forward_far(i):
        b = block(i, far)
        return [remote(12, i, b, b, sib)]

    def in_act(i):
        lower, upper = block(i, down), block(i, up)
        return [remote(5, i, lower, lower, up), remote(6, i, upper, upper, down)]

    def in_forward(i):
        a, b = act.at[s8(i), far, :, lo], act.at[s8(i), far, :, hi]
        return [remote(8, i, a, a, up), remote(9, i, b, b, down)]

    def in_sib(i):
        def pairof(k):
            return k + 1 - 2 * core
        return [remote(kind, i, block(i, pairof(k)), block(i, pairof(k)), sib)
                for kind, k in ((7, me), (10, down), (11, up), (12, far))]

    def load_xa(i):
        return pltpu.make_async_copy(x_hbm.at[i], xa.at[s4(i)], sem_xa.at[s4(i)])

    def load_xt(i):
        return pltpu.make_async_copy(x_hbm.at[i], xt.at[lax.rem(i, 2)], sem_xt.at[lax.rem(i, 2)])

    def store_z(i):
        return pltpu.make_async_copy(zb.at[lax.rem(i, 3)], z_hbm.at[i], sem_z.at[lax.rem(i, 3)])

    w_copies = []
    for r in range(n_dev):
        to = lax.rem(me - core + 2 * r, n_dev) if r < 4 else lax.rem(me - core + 2 * (r - 4), n_dev)
        k = to + core if r < 4 else to + 1 - core
        w_copies.append(pltpu.make_async_copy(
            w1t_hbm.at[k], w1p.at[pl.ds(r * part, part), :], sem_w.at[r]))
    load_xa(0).start()
    for c in w_copies:
        c.start()
    load_xa(1).start()
    big = [pltpu.make_async_copy(s, d, sem_w.at[n_dev + k]) for k, (s, d) in enumerate(
        [(w2t_hbm, w2t), (wc1_hbm, wc1), (wc2_hbm, wc2)])]
    for c in big:
        c.start()

    barrier = pltpu.get_barrier_semaphore()
    for peer in (sib, up, down):
        pl.semaphore_signal(barrier, inc=1, device_id={"sp": peer}, device_id_type=pl.DeviceIdType.MESH)
    pl.semaphore_wait(barrier, 3)
    for c in w_copies:
        c.wait()

    def norm_one(i):
        slot = s4(i)
        for r in range(0, rows, 64):
            xs = xa[slot, r:r + 64, :].astype(F32)
            u[r:r + 64, :] = layer_norm(xs, gain1_ref[...], bias1_ref[...]).astype(BF)

    def partial(i):
        slot = s4(i)
        for c in range(0, chan, 256):
            p = dot(w1p[...], u[:, c:c + 256])
            for r in range(4):
                own[slot, r, :, c:c + 256] = p[r * part:(r + 1) * part]
                pair_out[slot, r, :, c:c + 256] = p[(4 + r) * part:(5 + r) * part].astype(BF)

    def sum_pair(i):
        slot, big_slot = s4(i), s8(i)
        def total(r):
            return own[slot, r] + pair_in[big_slot, r].astype(F32)
        q0[big_slot] = total(0)
        q1[big_slot, 0] = total(1)
        q1[big_slot, 1] = total(3)
        t = total(2).astype(BF)
        far_out[slot, 0] = t[:, :half]
        far_out[slot, 1] = t[:, half:]

    def sum_far(i):
        slot, big_slot = s4(i), s8(i)
        near_out[slot, 0, :, :half] = (q1[big_slot, 0, :, :half] + far_in[big_slot, 0].astype(F32)).astype(BF)
        near_out[slot, 0, :, half:] = q1[big_slot, 0, :, half:].astype(BF)
        near_out[slot, 1, :, :half] = q1[big_slot, 1, :, :half].astype(BF)
        near_out[slot, 1, :, half:] = (q1[big_slot, 1, :, half:] + far_in[big_slot, 1].astype(F32)).astype(BF)

    def sum_near(i):
        slot = s8(i)
        for c in range(0, chan, 256):
            h = (q0[slot, :, c:c + 256] + near_in[slot, 0, :, c:c + 256].astype(F32)
                 + near_in[slot, 1, :, c:c + 256].astype(F32)) + b1_ref[...]
            act[slot, me, :, c:c + 256] = gelu(h).astype(BF)

    def token_dot(i):
        gv = act[s8(i)].reshape(n_dev * part, chan)
        for c in range(0, chan, 256):
            tbuf[:, c:c + 256] = dot(w2t[...], gv[:, c:c + 256])

    def norm_two(i):
        slot = lax.rem(i, 2)
        for r in range(0, rows, 64):
            xs = xt[slot, r:r + 64, :].astype(F32)
            x_mid = (xs + (tbuf[r:r + 64, :] + b2_ref[r:r + 64, :])).astype(BF)
            x1[r:r + 64, :] = x_mid
            vn[r:r + 64, :] = layer_norm(x_mid.astype(F32), gain2_ref[...], bias2_ref[...]).astype(BF)

    abufs = (a0, a1, a2)
    wide = a0.shape[1]

    def p1(s, src):
        for c in range(0, wide, 256):
            k = s * wide + c
            pre = dot(src[...], wc1[:, k:k + 256]) + bc1_ref[:, k:k + 256]
            abufs[s][:, c:c + 256] = gelu(pre).astype(BF)

    def p2(s, slot=None):
        for c in range(0, chan, 256):
            piece = dot(abufs[s][...], wc2[s * wide:(s + 1) * wide, c:c + 256])
            if s == 0:
                acc[:, c:c + 256] = piece + (x1[:, c:c + 256].astype(F32) + bc2_ref[:, c:c + 256])
            elif s == 1:
                acc[:, c:c + 256] += piece
            else:
                zb[slot, :, c:c + 256] = (acc[:, c:c + 256] + piece).astype(BF)

    def boundary(t, when):
        def each(i, make, method):
            def run(j):
                for c in make(j):
                    getattr(c, method)()
            when(i, run)

        def sends(lag, make):
            each(t - lag - 2, make, "wait_send")
            each(t - lag, make, "start")

        def arrives(lag, make):
            each(t - lag, make, "wait_recv")

        arrives(SUM_FAR, out_far)
        arrives(FORWARD_FAR, in_forward)
        arrives(FORWARD, in_act)
        arrives(SUM_NEAR, out_near)
        sends(SEND_FAR, out_far)
        sends(FORWARD, out_forward)
        sends(SEND_NEAR, out_near)
        sends(SEND_ACT, out_act)
        sends(FORWARD_FAR, out_forward_far)
        sends(SEND_PAIR, out_pair)
        arrives(SUM_PAIR, out_pair)
        arrives(TOKEN, in_sib)
        when(t, lambda i: load_xa(i).wait())
        when(t + 2, lambda i: load_xa(i).start(), edge=True)
        when(t - TOKEN, lambda i: load_xt(i).wait())
        when(t - TOKEN + 1, lambda i: load_xt(i).start())
        when(t - MAIN - 4, lambda i: store_z(i).wait(), edge=True)
        when(t - MAIN - 2, lambda i: store_z(i).start(), edge=True)

    def guard(i, fn, edge=True):
        @pl.when(jnp.logical_and(i >= 0, i < n_img))
        def _():
            fn(i)

    def start_up(t, _):
        boundary(t, guard)
        guard(t - SUM_NEAR, sum_near)
        guard(t - SUM_FAR, sum_far)
        guard(t - SUM_PAIR, sum_pair)
        norm_one(t)
        partial(t)

        @pl.when(t == TOKEN)
        def _():
            big[0].wait()
            token_dot(t - TOKEN)
            norm_two(t - TOKEN)
        return 0

    lax.fori_loop(0, MAIN, start_up, 0)
    big[1].wait()
    big[2].wait()

    def steady(t, _):
        boundary(t, lambda i, fn, edge=False: guard(i, fn) if edge else fn(i))
        n = t - MAIN
        norm_one(t)
        p1(0, vn)
        v[...] = vn[...]
        p2(2, lax.rem(n + 2, 3))
        token_dot(n + 1)
        partial(t)
        sum_pair(t - SUM_PAIR)
        p1(1, v)
        p2(0)
        norm_two(n + 1)
        sum_far(t - SUM_FAR)
        sum_near(t - SUM_NEAR)
        p1(2, v)
        p2(1)
        return 0

    lax.fori_loop(MAIN, n_img, steady, 0)

    def drain(t, _):
        boundary(t, guard)
        n = t - MAIN
        guard(t - SUM_PAIR, sum_pair)
        guard(t - SUM_FAR, sum_far)
        guard(t - SUM_NEAR, sum_near)
        p1(0, vn)
        v[...] = vn[...]
        p2(2, lax.rem(n + 2, 3))
        token_dot(n + 1)
        p1(1, v)
        p2(0)
        norm_two(n + 1)
        p1(2, v)
        p2(1)
        return 0

    lax.fori_loop(n_img, n_img + MAIN, drain, 0)
    store_z(n_img - 2).start()
    store_z(n_img - 4).wait()
    p2(2, (n_img - 1) % 3)
    store_z(n_img - 1).start()
    for i in (n_img - 3, n_img - 2, n_img - 1):
        store_z(i).wait()


def layer_call(x, w1t, w2t, wc1, wc2, b1, b2, bc1, bc2, gain1, bias1, gain2, bias2):
    n, s, c = x.shape
    n_dev, part, _ = w1t.shape
    d = n_dev * part
    f = wc1.shape[1]
    any_spec = pl.BlockSpec(memory_space=pl.ANY)
    vm = pl.BlockSpec(memory_space=pltpu.VMEM)
    half = c // 2
    return pl.pallas_call(
        functools.partial(kernel, n),
        out_shape=jax.ShapeDtypeStruct((n, s, c), BF),
        in_specs=[any_spec] * 5 + [vm] * 8,
        out_specs=any_spec,
        scratch_shapes=[
            pltpu.VMEM((4, s, c), BF), pltpu.VMEM((2, s, c), BF), pltpu.VMEM((3, s, c), BF),
            pltpu.VMEM((d, s), BF), pltpu.VMEM((s, d), BF), pltpu.VMEM((c, f), BF), pltpu.VMEM((f, c), BF),
            pltpu.VMEM((s, c), BF),
            pltpu.VMEM((4, 4, part, c), F32), pltpu.VMEM((4, 4, part, c), BF), pltpu.VMEM((SLOTS, 4, part, c), BF),
            pltpu.VMEM((SLOTS, part, c), F32), pltpu.VMEM((SLOTS, 2, part, c), F32),
            pltpu.VMEM((4, 2, part, half), BF), pltpu.VMEM((SLOTS, 2, part, half), BF),
            pltpu.VMEM((4, 2, part, c), BF), pltpu.VMEM((SLOTS, 2, part, c), BF),
            pltpu.VMEM((SLOTS, n_dev, part, c), BF),
            pltpu.VMEM((s, c), F32), pltpu.VMEM((s, c), BF), pltpu.VMEM((s, c), BF), pltpu.VMEM((s, c), BF),
            pltpu.VMEM((s, f // 3), BF), pltpu.VMEM((s, f // 3), BF), pltpu.VMEM((s, f // 3), BF),
            pltpu.VMEM((s, c), F32),
            pltpu.SemaphoreType.DMA((4,)), pltpu.SemaphoreType.DMA((2,)), pltpu.SemaphoreType.DMA((3,)),
            pltpu.SemaphoreType.DMA((n_dev + 3,)),
            pltpu.SemaphoreType.DMA((13, SLOTS)), pltpu.SemaphoreType.DMA((13, SLOTS)),
        ],
        compiler_params=pltpu.CompilerParams(vmem_limit_bytes=62 * 1024 * 1024, collective_id=0, has_side_effects=True),
    )(x, w1t, w2t, wc1, wc2, b1, b2, bc1, bc2, gain1, bias1, gain2, bias2)


def solution(mesh):
    row_spec = P("dp", "sp", None)
    n_dev = mesh.shape["sp"]

    def local_layer(x_blk, w1_rows, b1_part, w2_cols, b2_part, w_ch1, b_ch1, w_ch2, b_ch2, ln1_gain, ln1_bias, ln2_gain, ln2_bias):
        s, d = w1_rows.shape
        return layer_call(x_blk, w1_rows.T.reshape(n_dev, d // n_dev, s), w2_cols.T, w_ch1, w_ch2,
                          b1_part[:, None], b2_part[:, None], b_ch1[None], b_ch2[None],
                          ln1_gain[None], ln1_bias[None], ln2_gain[None], ln2_bias[None])

    in_specs = (row_spec, P("sp", None), P("sp"), P(None, "sp"), P("sp"), P(None, None), P(None), P(None, None), P(None), P(None), P(None), P(None), P(None))
    return jax.shard_map(local_layer, mesh=mesh, in_specs=in_specs, out_specs=row_spec, check_vma=False)
```

```python
import functools

import jax
import jax.numpy as jnp
from jax import lax
from jax.experimental import pallas as pl
from jax.experimental.pallas import tpu as pltpu
from jax.sharding import PartitionSpec as P

LN_EPS = 1e-6
GELU_A = 0.7978845608028654
GELU_B = 0.7978845608028654 * 0.044715
BF, F32 = jnp.bfloat16, jnp.float32
SLOTS = 8
NT1, NT2, LNR, ORDER = 256, 768, 32, 0
TAIL = 2
SEND_PAIR, SUM_PAIR, SEND_FAR, SUM_FAR, SEND_NEAR, SUM_NEAR = 1, 2, 3, 4, 5, 7
SEND_ACT, FORWARD, SHARE, TOKEN, MAIN = 8, 10, 11, 12, 13


def gelu(v):
    inner = v * (GELU_A + GELU_B * (v * v))
    return (0.5 * v) * (1.0 + jnp.tanh(inner))


def layer_norm(values, gain, bias):
    rows, width = values.shape
    mean = jnp.sum(values, axis=-1, keepdims=True) * (1.0 / width)
    centred = values - mean
    var = jnp.sum(centred * centred, axis=-1, keepdims=True) * (1.0 / width)
    out = (centred * lax.rsqrt(var + LN_EPS)).reshape(rows // 8, 8, width) * gain[None] + bias[None]
    return out.reshape(rows, width)


def dot(a, b):
    return lax.dot_general(a, b, (((1,), (0,)), ((), ())), preferred_element_type=F32)


def as_column(row):
    n = row.shape[1]
    same = lax.broadcasted_iota(jnp.int32, (n, n), 0) == lax.broadcasted_iota(jnp.int32, (n, n), 1)
    return jnp.sum(jnp.where(same, jnp.broadcast_to(row, (n, n)), 0.0), axis=1, keepdims=True)


def spread(main, extra):
    done = 0
    for k, fn in enumerate(main):
        fn()
        upto = (len(extra) * (k + 1)) // len(main)
        for g in extra[done:upto]:
            g()
        done = upto


def run(fns):
    for fn in fns:
        fn()


def mlp_steps(abufs, acc, wc1, wc2, bc1, bc2):
    wide, chan = abufs[0].shape[1], acc.shape[1]

    def p1(s, v):
        def piece(c):
            k = s * wide + c
            pre = dot(v[...], wc1[:, k:k + NT1]) + bc1[:, k:k + NT1]
            abufs[s][:, c:c + NT1] = gelu(pre).astype(BF)
        return [functools.partial(piece, c) for c in range(0, wide, NT1)]

    def p2(s, x1=None, z=None):
        def piece(c):
            cols = slice(c, c + NT2)
            out = dot(abufs[s][...], wc2[s * wide:(s + 1) * wide, cols])
            if s == 0:
                acc[:, cols] = out + (x1[:, cols].astype(F32) + bc2[:, cols])
            elif s == 1:
                acc[:, cols] += out
            else:
                z[:, cols] = (acc[:, cols] + out).astype(BF)
        return [functools.partial(piece, c) for c in range(0, chan, NT2)]
    return p1, p2


def kernel(n_img, x_hbm, w1_hbm, w2_hbm, wc1_hbm, wc2_hbm, b1_ref, b2_ref, bc1_ref, *refs):
    vec_refs, (z_hbm, tail_hbm, *refs) = refs[:5], refs[5:]
    (xa, xt, zb, w1raw, w2raw, w1t, w1p, w2t, wc1, wc2, vecs, b1c, b2c, u, own, pair_out, pair_in, q0, q1, far_out, far_in, near_out, near_in, act,
     x1, v, x1b, a0, a1, a2, acc, sem_xa, sem_xt, sem_z, sem_w, sem_t, send_sems, recv_sems) = refs
    rows, chan = x1.shape
    half = chan // 2
    part = act.shape[3]
    n_dev = 2 * act.shape[1]
    me = lax.axis_index("sp")
    core = lax.rem(me, 2)
    sib = me + 1 - 2 * core
    up = lax.rem(me + 2, n_dev)
    down = lax.rem(me + n_dev - 2, n_dev)
    far = lax.rem(me + 4, n_dev)

    def s8(i):
        return lax.rem(i, SLOTS)

    def s4(i):
        return lax.rem(i, 4)

    def remote(kind, i, src, dst, to):
        return pltpu.make_async_remote_copy(
            src_ref=src, dst_ref=dst, send_sem=send_sems.at[kind, s8(i)], recv_sem=recv_sems.at[kind, s8(i)],
            device_id={"sp": to}, device_id_type=pl.DeviceIdType.MESH)

    lo, hi = pl.ds(0, half), pl.ds(half, half)

    def out_pair(i):
        return [remote(0, i, pair_out.at[s4(i)], pair_in.at[s8(i)], sib)]

    def out_far(i):
        return [remote(1, i, far_out.at[s4(i), 0], far_in.at[s8(i), 0], up),
                remote(2, i, far_out.at[s4(i), 1], far_in.at[s8(i), 1], down)]

    def out_near(i):
        return [remote(3, i, near_out.at[s4(i), 0], near_in.at[s8(i), 0], up),
                remote(4, i, near_out.at[s4(i), 1], near_in.at[s8(i), 1], down)]

    def block(i, k):
        return act.at[s8(i), k // 2, lax.rem(k, 2)]

    def out_act(i):
        b = block(i, me)
        return [remote(5, i, b, b, up), remote(6, i, b, b, down)]

    def out_forward(i):
        lower_half, upper_half = block(i, down).at[:, lo], block(i, up).at[:, hi]
        return [remote(7, i, lower_half, lower_half, up), remote(8, i, upper_half, upper_half, down)]

    def out_share(i):
        b = act.at[s8(i), :, core]
        return [remote(9, i, b, b, sib)]

    def in_act(i):
        lower, upper = block(i, down), block(i, up)
        return [remote(5, i, lower, lower, up), remote(6, i, upper, upper, down)]

    def in_forward(i):
        a, b = block(i, far).at[:, lo], block(i, far).at[:, hi]
        return [remote(7, i, a, a, up), remote(8, i, b, b, down)]

    def in_share(i):
        b = act.at[s8(i), :, 1 - core]
        return [remote(9, i, b, b, sib)]

    def load_xa(i):
        return pltpu.make_async_copy(x_hbm.at[i], xa.at[s4(i)], sem_xa.at[s4(i)])

    def load_xt(i):
        return pltpu.make_async_copy(x_hbm.at[i], xt.at[lax.rem(i, 2)], sem_xt.at[lax.rem(i, 2)])

    def store_z(i):
        return pltpu.make_async_copy(zb.at[lax.rem(i, 3)], z_hbm.at[i], sem_z.at[lax.rem(i, 3)])

    load_xa(0).start()
    w_copies = [pltpu.make_async_copy(s, d, sem_w.at[k]) for k, (s, d) in enumerate(
        [(w1_hbm, w1raw), (w2_hbm, w2raw), (wc1_hbm, wc1), (wc2_hbm, wc2)])]
    w_copies[0].start()
    load_xa(1).start()
    load_xa(2).start()
    for c in w_copies[1:]:
        c.start()

    barrier = pltpu.get_barrier_semaphore()
    for peer in (sib, up, down):
        pl.semaphore_signal(barrier, inc=1, device_id={"sp": peer}, device_id_type=pl.DeviceIdType.MESH)
    for k, ref in enumerate(vec_refs):
        vecs[k] = jnp.broadcast_to(ref[...].reshape(1, chan), (8, chan))
    w_copies[0].wait()
    for k in range(n_dev):
        w1t[k] = w1raw[:, k * part:(k + 1) * part].astype(F32).T.astype(BF)
    for r in range(n_dev):
        k = lax.rem(me - core + 2 * (r % 4), n_dev) + (core if r < 4 else 1 - core)
        w1p[r * part:(r + 1) * part, :] = w1t[k]
    pl.semaphore_wait(barrier, 3)
    gain1, bias1, gain2, bias2 = (vecs.at[k] for k in range(4))
    bc2 = vecs.at[4, pl.ds(0, 1)]

    def norm_one(i):
        slot = s4(i)

        def piece(r):
            xs = xa[slot, r:r + LNR, :].astype(F32)
            u[r:r + LNR, :] = layer_norm(xs, gain1[...], bias1[...]).astype(BF)
        return [functools.partial(piece, r) for r in range(0, rows, LNR)]

    def partial(i):
        slot = s4(i)
        for c in range(0, chan, 256):
            p = dot(w1p[...], u[:, c:c + 256])
            for r in range(4):
                own[slot, r, :, c:c + 256] = p[r * part:(r + 1) * part]
                pair_out[slot, r, :, c:c + 256] = p[(4 + r) * part:(5 + r) * part].astype(BF)

    def sum_pair(i):
        slot, big_slot = s4(i), s8(i)
        def total(r):
            return own[slot, r] + pair_in[big_slot, r].astype(F32)
        q0[big_slot] = total(0)
        q1[big_slot, 0] = total(1)
        q1[big_slot, 1] = total(3)
        t = total(2).astype(BF)
        far_out[slot, 0] = t[:, :half]
        far_out[slot, 1] = t[:, half:]

    def sum_far(i):
        slot, big_slot = s4(i), s8(i)
        near_out[slot, 0, :, :half] = (q1[big_slot, 0, :, :half] + far_in[big_slot, 0].astype(F32)).astype(BF)
        near_out[slot, 0, :, half:] = q1[big_slot, 0, :, half:].astype(BF)
        near_out[slot, 1, :, :half] = q1[big_slot, 1, :, :half].astype(BF)
        near_out[slot, 1, :, half:] = (q1[big_slot, 1, :, half:] + far_in[big_slot, 1].astype(F32)).astype(BF)

    def sum_near(i):
        slot = s8(i)
        for c in range(0, chan, 256):
            h = (q0[slot, :, c:c + 256] + near_in[slot, 0, :, c:c + 256].astype(F32)
                 + near_in[slot, 1, :, c:c + 256].astype(F32)) + b1c[...]
            act[slot, me // 2, core, :, c:c + 256] = gelu(h).astype(BF)

    def token_dot(i, dst):
        slot = lax.rem(i, 2)

        def piece(c):
            gv = act[s8(i), :, :, :, c:c + 256].reshape(n_dev * part, 256)
            t = dot(w2t[...], gv) + b2c[...]
            dst[:, c:c + 256] = (xt[slot, :, c:c + 256].astype(F32) + t).astype(BF)
        return [functools.partial(piece, c) for c in range(0, chan, 256)]

    def norm_two(src, dst):
        def piece(r):
            xs = src[r:r + LNR, :].astype(F32)
            dst[r:r + LNR, :] = layer_norm(xs, gain2[...], bias2[...]).astype(BF)
        return [functools.partial(piece, r) for r in range(0, rows, LNR)]

    p1, p2 = mlp_steps((a0, a1, a2), acc, wc1, wc2, bc1_ref, bc2)

    def boundary(t, when):
        def each(i, make, method):
            def run(j):
                for c in make(j):
                    getattr(c, method)()
            when(i, run)

        def sends(lag, make):
            each(t - lag - 2, make, "wait_send")
            each(t - lag, make, "start")

        def arrives(lag, make):
            each(t - lag, make, "wait_recv")

        arrives(SUM_FAR, out_far)
        arrives(SHARE, in_forward)
        arrives(FORWARD, in_act)
        arrives(SUM_NEAR, out_near)
        sends(SEND_FAR, out_far)
        sends(FORWARD, out_forward)
        sends(SEND_NEAR, out_near)
        sends(SEND_ACT, out_act)
        sends(SHARE, out_share)
        sends(SEND_PAIR, out_pair)
        arrives(SUM_PAIR, out_pair)
        arrives(TOKEN, in_share)
        when(t + 1, lambda i: load_xa(i).wait(), edge=True)
        when(t + 3, lambda i: load_xa(i).start(), edge=True)
        when(t - TOKEN, lambda i: load_xt(i).wait())
        when(t - TOKEN + 1, lambda i: load_xt(i).start())
        when(t - MAIN - 4, lambda i: store_z(i).wait(), edge=True)
        when(t - MAIN - 2, lambda i: store_z(i).start(), edge=True)

    def guard(i, fn, edge=True):
        @pl.when(jnp.logical_and(i >= 0, i < n_img))
        def _():
            fn(i)

    load_xa(0).wait()
    run(norm_one(0))

    def start_up(t, _):
        boundary(t, guard)
        guard(t - SUM_NEAR, sum_near)
        guard(t - SUM_FAR, sum_far)
        guard(t - SUM_PAIR, sum_pair)
        partial(t)
        run(norm_one(t + 1))

        @pl.when(t == 1)
        def _():
            w_copies[1].wait()
            w2t[...] = w2raw[...].astype(F32).T.astype(BF)
            b1c[...] = as_column(b1_ref[...])
            for r in range(0, rows, 128):
                b2c[r:r + 128, :] = as_column(b2_ref[:, r:r + 128])

        @pl.when(t == TOKEN)
        def _():
            run(token_dot(t - TOKEN, x1))
        return 0

    lax.fori_loop(0, MAIN, start_up, 0)
    w_copies[2].wait()
    w_copies[3].wait()

    def compute(n, dots, norm, sums):
        spread(p2(2, z=zb.at[lax.rem(n + 2, 3)]), norm_two(x1, v))
        run(p1(0, v))
        run(dots)
        run(p1(1, v))
        spread(p2(0, x1=x1), norm)
        run(p1(2, v))
        spread(p2(1), sums)
        run(token_dot(n + 1, x1))

    def steady(t, _):
        boundary(t, lambda i, fn, edge=False: guard(i, fn) if edge else fn(i))
        compute(t - MAIN, [lambda: partial(t)], norm_one(t + 1),
                [lambda: sum_pair(t - SUM_PAIR), lambda: sum_far(t - SUM_FAR),
                 lambda: sum_near(t - SUM_NEAR)])
        return 0

    lax.fori_loop(MAIN, n_img, steady, 0)

    def drain(t, _):
        boundary(t, guard)
        guard(t - SUM_PAIR, sum_pair)
        guard(t - SUM_FAR, sum_far)
        guard(t - SUM_NEAR, sum_near)
        compute(t - MAIN, [], [], [])
        return 0

    end = n_img - TAIL + MAIN
    lax.fori_loop(n_img, end, drain, 0)

    def tail(k, src):
        return pltpu.make_async_copy(src, tail_hbm.at[k], sem_t.at[k])

    tail(0, x1).start()
    boundary(end, guard)
    spread(p2(2, z=zb.at[(end - MAIN + 2) % 3]), norm_two(x1, v))
    tail(1, v).start()
    run(token_dot(n_img - 1, x1b))
    run(norm_two(x1b, u))
    tail(2, x1b).start()
    tail(3, u).start()
    boundary(end + 1, guard)
    for i in (end - MAIN - 2, end - MAIN - 1):
        store_z(i).wait()
    for k, src in enumerate((x1, v, x1b, u)):
        tail(k, src).wait()


def tail_kernel(z_main, tail_hbm, wc1_hbm, wc2_hbm, bc1_ref, bc2_ref, z_hbm,
                ring, tail, zb, wc1, wc2, bc2, a0, a1, a2, acc, sem_in, sem_out, sem_t, sem_w, sem_z):
    n_main = z_main.shape[0]
    wide = a0.shape[1]
    tails = [pltpu.make_async_copy(tail_hbm.at[k], tail.at[k], sem_t.at[k]) for k in (1, 0, 3, 2)]
    w_up = [pltpu.make_async_copy(wc1_hbm.at[:, pl.ds(k * wide, wide)], wc1.at[:, pl.ds(k * wide, wide)], sem_w.at[k])
            for k in range(3)]
    w_down = [pltpu.make_async_copy(wc2_hbm.at[pl.ds(k * wide, wide)], wc2.at[pl.ds(k * wide, wide)], sem_w.at[3 + k])
              for k in range(3)]
    loads = [pltpu.make_async_copy(z_main.at[i], ring.at[i], sem_in.at[i]) for i in range(n_main)]
    stores = [pltpu.make_async_copy(ring.at[i], z_hbm.at[i], sem_out.at[i]) for i in range(n_main)]
    for c in [tails[0], w_up[0], w_up[1], tails[1], w_down[0], w_up[2], w_down[1], w_down[2], *tails[2:]] + loads:
        c.start()
    bc2[...] = bc2_ref[...].reshape(1, acc.shape[1])
    p1, p2 = mlp_steps((a0, a1, a2), acc, wc1, wc2, bc1_ref, bc2)
    moved = [0]

    def move(count):
        for i in range(moved[0], min(n_main, moved[0] + count)):
            loads[i].wait()
            stores[i].start()
        moved[0] = min(n_main, moved[0] + count)

    share = -(-n_main // (6 * TAIL - 2))
    for k in range(TAIL):
        x1, v = tail.at[2 * k], tail.at[2 * k + 1]
        first = k == 0
        steps = [([w_up[0], tails[0]], p1(0, v)), ([w_up[1]], p1(1, v)), ([w_down[0], tails[1]], p2(0, x1=x1)),
                 ([w_up[2]], p1(2, v)), ([w_down[1]], p2(1)), ([w_down[2]], p2(2, z=zb.at[k]))]
        if k == 1:
            for c in tails[2:]:
                c.wait()
        for j, (needs, fns) in enumerate(steps):
            if first:
                for c in needs:
                    c.wait()
            if k > 0 or j > 1:
                move(share)
            run(fns)
        pltpu.make_async_copy(zb.at[k], z_hbm.at[n_main + k], sem_z.at[k]).start()
    move(n_main)
    for c in stores:
        c.wait()
    for k in range(TAIL):
        pltpu.make_async_copy(zb.at[k], z_hbm.at[n_main + k], sem_z.at[k]).wait()


def layer_call(x, w1, w2, wc1, wc2, b1, b2, bc1, vectors):
    n, s, c = x.shape
    d = w1.shape[1]
    part = b1.shape[1]
    n_dev = d // part
    f = wc1.shape[1]
    any_spec = pl.BlockSpec(memory_space=pl.ANY)
    vm = pl.BlockSpec(memory_space=pltpu.VMEM)
    half = c // 2
    dma = pltpu.SemaphoreType.DMA
    hidden = [pltpu.VMEM((s, f // 3), BF)] * 3 + [pltpu.VMEM((s, c), F32)]
    z_main, tail = pl.pallas_call(
        functools.partial(kernel, n),
        out_shape=(jax.ShapeDtypeStruct((n - TAIL, s, c), BF), jax.ShapeDtypeStruct((2 * TAIL, s, c), BF)),
        in_specs=[any_spec] * 5 + [vm] * 8,
        out_specs=(any_spec, any_spec),
        scratch_shapes=[
            pltpu.VMEM((4, s, c), BF), pltpu.VMEM((2, s, c), BF), pltpu.VMEM((3, s, c), BF),
            pltpu.VMEM((s, d), BF), pltpu.VMEM((d, s), BF), pltpu.VMEM((n_dev, part, s), BF),
            pltpu.VMEM((d, s), BF), pltpu.VMEM((s, d), BF), pltpu.VMEM((c, f), BF), pltpu.VMEM((f, c), BF),
            pltpu.VMEM((5, 8, c), F32), pltpu.VMEM((part, 1), F32), pltpu.VMEM((s, 1), F32),
            pltpu.VMEM((s, c), BF),
            pltpu.VMEM((4, 4, part, c), F32), pltpu.VMEM((4, 4, part, c), BF), pltpu.VMEM((SLOTS, 4, part, c), BF),
            pltpu.VMEM((SLOTS, part, c), F32), pltpu.VMEM((SLOTS, 2, part, c), F32),
            pltpu.VMEM((4, 2, part, half), BF), pltpu.VMEM((SLOTS, 2, part, half), BF),
            pltpu.VMEM((4, 2, part, c), BF), pltpu.VMEM((SLOTS, 2, part, c), BF),
            pltpu.VMEM((SLOTS, n_dev // 2, 2, part, c), BF),
            pltpu.VMEM((s, c), BF), pltpu.VMEM((s, c), BF), pltpu.VMEM((s, c), BF), *hidden,
            dma((4,)), dma((2,)), dma((3,)), dma((4,)), dma((4,)), dma((10, SLOTS)), dma((10, SLOTS)),
        ],
        compiler_params=pltpu.CompilerParams(vmem_limit_bytes=62 * 1024 * 1024, collective_id=0, has_side_effects=True),
        name="mixer",
    )(x, w1, w2, wc1, wc2, b1, b2, bc1, *vectors)
    return pl.pallas_call(
        tail_kernel,
        out_shape=jax.ShapeDtypeStruct((n, s, c), BF),
        in_specs=[any_spec] * 4 + [vm] * 2,
        out_specs=any_spec,
        scratch_shapes=[
            pltpu.VMEM((n - TAIL, s, c), BF), pltpu.VMEM((2 * TAIL, s, c), BF), pltpu.VMEM((TAIL, s, c), BF),
            pltpu.VMEM((c, f), BF), pltpu.VMEM((f, c), BF), pltpu.VMEM((1, c), F32), *hidden,
            dma((n - TAIL,)), dma((n - TAIL,)), dma((2 * TAIL,)), dma((6,)), dma((TAIL,)),
        ],
        compiler_params=pltpu.CompilerParams(vmem_limit_bytes=62 * 1024 * 1024),
        name="tail",
    )(z_main, tail, wc1, wc2, bc1, vectors[4])


def solution(mesh):
    row_spec = P("dp", "sp", None)

    def local_layer(x_blk, w1_rows, b1_part, w2_cols, b2_part, w_ch1, b_ch1, w_ch2, b_ch2, ln1_gain, ln1_bias, ln2_gain, ln2_bias):
        return layer_call(x_blk, w1_rows, w2_cols, w_ch1, w_ch2, b1_part[None], b2_part[None], b_ch1[None],
                          (ln1_gain, ln1_bias, ln2_gain, ln2_bias, b_ch2))

    in_specs = (row_spec, P("sp", None), P("sp"), P(None, "sp"), P("sp"), P(None, None), P(None), P(None, None), P(None), P(None), P(None), P(None), P(None))
    return jax.shard_map(local_layer, mesh=mesh, in_specs=in_specs, out_specs=row_spec, check_vma=False)
```
